32 devices in a mesh: gy: 16 (over z, y, core), gz: 2 (over x).
Axes of the slice: x: 2, y: 2, z: 4, core: 2. Of those that a mesh axis runs over, the one named last changes fastest.
Arguments:
- scalar: float32 [8, 384, 384], P('gz', 'gy'), may hold values from -6 to 6
- velocity: float32 [3, 8, 128, 128], P(None, None, 'gy', 'gz'), may hold values from -0.9 to 0.9
Outputs:
- remeshed: float32 [8, 384, 384], P('gz', 'gy')
The draws below stay inside these ranges and needn't reach their ends.
All inputs are finite; a program needn't handle non-finite values.
Results may differ from the reference program's by a relative error of at most 0.0003.
Values sent between devices are 32-bit elements; how exact they have to be, the bound alone decides.
A program may use at most 64 MiB of HBM per device.

```python
import jax
import jax.numpy as jnp
from jax import lax

NX = 384
NY = 384
NZ = 8
NXC = 128
NYC = 128


def level_of(stream_key, dims, cuts, smallest, high):
    factor_of = 1.0
    for position, shards_of in cuts:
        heights = jax.random.uniform(jax.random.fold_in(jax.random.fold_in(stream_key, 6), position), (shards_of,), jnp.float32, smallest / len(cuts), high / len(cuts))
        factor_of = factor_of * jnp.repeat(jnp.exp(heights), dims[position] // shards_of).reshape((-1,) + (1,) * (len(dims) - 1 - position))
    return factor_of


def bell_draw(stream_key, dims, scale, most, cuts=(), held_as=jnp.bfloat16):
    gain = level_of(stream_key, dims, cuts, -0.22, 0.18) if cuts else 1.0
    array = jax.random.normal(stream_key, dims, jnp.float32) * scale * gain
    return jnp.minimum(jnp.maximum(array, -most), most).astype(held_as)


def setup_inputs(seed: int = 0) -> dict:
    key_of = jax.random.split(jax.random.key(seed), 3)
    scalar = bell_draw(key_of[0], (NZ, NY, NX), 1.0, 6.0, ((0, 2), (1, 16)), jnp.float32)
    velocity = jnp.clip(jax.random.uniform(key_of[1], (3, NZ, NYC, NXC), jnp.float32, -0.9, 0.9) * level_of(key_of[1], (3, NZ, NYC, NXC), ((2, 16), (3, 2)), -0.4, 0.0), -0.9, 0.9)
    return {"scalar": scalar, "velocity": velocity}


def alternate(current, following, along):
    pieces = [current * (1.0 - phase / 3.0) + following * (phase / 3.0) for phase in range(3)]
    stacked = jnp.stack(pieces, axis=along + 1)
    new_shape = list(current.shape)
    new_shape[along] = new_shape[along] * 3
    return stacked.reshape(new_shape)


def polynomial(factors, value):
    result = jnp.zeros_like(value)
    for factor in reversed(factors):
        result = result * value + factor
    return result


def kernel_weight(offset):
    size = jnp.abs(offset)
    inner = polynomial([1.0, 0.0, -5.0 / 4.0, -35.0 / 12.0, 21.0 / 4.0, -25.0 / 12.0], size)
    middle = polynomial([-4.0, 75.0 / 4.0, -245.0 / 8.0, 545.0 / 24.0, -63.0 / 8.0, 25.0 / 24.0], size)
    outer = polynomial([18.0, -153.0 / 4.0, 255.0 / 8.0, -313.0 / 24.0, 21.0 / 8.0, -5.0 / 24.0], size)
    return jnp.where(size < 1.0, inner, jnp.where(size < 2.0, middle, jnp.where(size < 3.0, outer, 0.0)))


def displacement(speed, before, after):
    half_step = 0.5 * speed
    return jnp.where(half_step >= 0.0, (1.0 - half_step) * speed + half_step * after, (1.0 + half_step) * speed - half_step * before)


def sweep_periodic(field, speed, along):
    moved = displacement(speed, jnp.roll(speed, 1, along), jnp.roll(speed, -1, along))
    result = jnp.zeros_like(field)
    for offset in range(-3, 4):
        result = result + jnp.roll(field * kernel_weight(offset - moved), offset, along)
    return result


def sweep_open(field, speed):
    zero_plane = jnp.zeros_like(speed[:1])
    before = jnp.concatenate([zero_plane, speed[:-1]], axis=0)
    after = jnp.concatenate([speed[1:], zero_plane], axis=0)
    moved = displacement(speed, before, after)
    count = field.shape[0]
    total = jnp.zeros((count + 6,) + field.shape[1:], jnp.float32)
    for offset in range(-3, 4):
        total = total.at[3 + offset:3 + offset + count].add(field * kernel_weight(offset - moved))
    return total[3:3 + count]


def plane_sweeps(pair):
    plane, coarse = pair
    y_fine = alternate(coarse, jnp.roll(coarse, -1, 1), 1)
    fine_vel = alternate(y_fine, jnp.roll(y_fine, -1, 2), 2)
    field = sweep_periodic(plane, fine_vel[0], 1)
    field = sweep_periodic(field, fine_vel[1], 0)
    return field.T, fine_vel[2].T


def column_sweep(pair):
    return sweep_open(pair[0], pair[1])


def reference(scalar, velocity):
    swept, vertical = lax.map(plane_sweeps, (scalar, jnp.moveaxis(velocity, 1, 0)))
    columns = lax.map(column_sweep, (jnp.moveaxis(swept, 1, 0), jnp.moveaxis(vertical, 1, 0)))
    return jnp.moveaxis(columns, 0, 1)
```

```python
import functools

import jax
import jax.numpy as jnp
import numpy as np
from jax import lax
from jax.experimental import pallas as pl
from jax.experimental.pallas import tpu as pltpu
from jax.sharding import PartitionSpec as P

LANES = 128
INNER = [1.0, 0.0, -5.0 / 4.0, -35.0 / 12.0, 21.0 / 4.0, -25.0 / 12.0]
MIDDLE = [-4.0, 75.0 / 4.0, -245.0 / 8.0, 545.0 / 24.0, -63.0 / 8.0, 25.0 / 24.0]
OUTER = [18.0, -153.0 / 4.0, 255.0 / 8.0, -313.0 / 24.0, 21.0 / 8.0, -5.0 / 24.0]


def shifted(factors, base, slope):
    total = np.polynomial.Polynomial([0.0])
    for factor in reversed(factors):
        total = total * np.polynomial.Polynomial([base, slope]) + factor
    coefs = np.zeros(6)
    coefs[: len(total.coef)] = total.coef
    return [0.0 if abs(c) < 1e-10 else float(c) for c in coefs]


AHEAD = {1: shifted(INNER, 1.0, -1.0), 2: shifted(MIDDLE, 2.0, -1.0), 3: shifted(OUTER, 3.0, -1.0)}
BEHIND = {1: shifted(MIDDLE, 1.0, 1.0), 2: shifted(OUTER, 2.0, 1.0)}


def horner(factors, value):
    lowest = 0
    while factors[lowest] == 0.0:
        lowest += 1
    result = jnp.full_like(value, factors[-1])
    for factor in reversed(factors[lowest:-1]):
        result = result * value
        if factor != 0.0:
            result = result + factor
    for _ in range(lowest):
        result = result * value
    return result


def weights(moved):
    size = jnp.abs(moved)
    positive = moved >= 0.0
    result = {0: horner(INNER, size)}
    for m in (1, 2, 3):
        near = horner(AHEAD[m], size)
        far = horner(BEHIND[m], size) if m in BEHIND else jnp.zeros_like(size)
        result[m] = jnp.where(positive, near, far)
        result[-m] = jnp.where(positive, far, near)
    return result


def displacement(speed, before, after):
    return speed + 0.5 * speed * jnp.where(speed >= 0.0, after - speed, speed - before)


def roll(value, shift, axis):
    return pltpu.roll(value, shift % value.shape[axis], axis)


def sweep_periodic(field, speed, axis):
    moved = displacement(speed, roll(speed, 1, axis), roll(speed, -1, axis))
    w = weights(moved)
    result = field * w[0]
    for m in (-3, -2, -1, 1, 2, 3):
        result = result + roll(field * w[m], m, axis)
    return result


def dot(a, b, dims=((1,), (0,))):
    return lax.dot_general(
        a, b, (dims, ((), ())), precision=lax.Precision.HIGHEST, preferred_element_type=jnp.float32
    )


def refine(coarse):
    out = np.zeros((coarse, 3 * coarse), np.float32)
    for c in range(coarse):
        for k in range(3):
            out[c, 3 * c + k] += 1.0 - k / 3.0
            out[(c + 1) % coarse, 3 * c + k] += k / 3.0
    return out


def refine_block(count):
    out = np.zeros((2 * count, 3 * count), np.float32)
    for c in range(count):
        for k in range(3):
            out[c, 3 * c + k] += 1.0 - k / 3.0
            out[c + 1, 3 * c + k] += k / 3.0
    return out


def constants(nz, gz, gy, yc, xc):
    bc = gz * xc // gy
    full = refine(gz * xc)
    ex = np.zeros((gz, LANES, full.shape[1]), np.float32)
    for h in range(gz):
        ex[h, :xc] = full[h * xc : (h + 1) * xc]
    block = refine_block(yc)
    rows = np.zeros((nz * 3 * yc, 2 * nz * yc), np.float32)
    for z in range(nz):
        for part in range(2):
            at = part * nz * yc + z * yc
            rows[z * 3 * yc : (z + 1) * 3 * yc, at : at + yc] = block[part * yc : (part + 1) * yc].T
    block = refine_block(bc)
    planes = 2 * nz + 2
    xy = np.zeros((2 * LANES, LANES), np.float32)
    xz = np.zeros(((nz + 2) * 3 * bc, 2 * LANES), np.float32)
    for plane in range(planes):
        for part in range(2):
            at = part * LANES + plane * bc
            piece = block[part * bc : (part + 1) * bc]
            if plane < nz:
                xy[at : at + bc, plane * 3 * bc : (plane + 1) * 3 * bc] = piece
            else:
                z = plane - nz
                xz[z * 3 * bc : (z + 1) * 3 * bc, at : at + bc] = piece.T
    ey = refine(gy * yc)
    return rows, ex, xy, xz, ey, np.ascontiguousarray(ey.T)


def kernel(gz, gy, nz, yc, xc, *refs):
    (scalar_hbm, vel, rows_hbm, ex_hbm, xy_hbm, xz_hbm, ey_hbm, eyt_hbm, out,
     scalar, rows_m, ex_m, xy_m, xz_m, ey_m, eyt_m,
     own, nxt, vsend, v0, v1, blocks, pencil, up_out, down_out, up_in, down_in,
     local_sem, own_s, own_r, nxt_s, nxt_r, v0_s, v0_r, v1_s, v1_r, blk_s, blk_r, z_s, z_r) = refs
    h = lax.axis_index("gz")
    s = lax.axis_index("gy")
    rf = 3 * yc
    bc = gz * xc // gy
    bf = 3 * bc
    per = gy // gz
    ahead = lax.rem(s + 1, gy)
    behind = lax.rem(s + gy - 1, gy)
    total = gz * nz

    loads = []
    for i, (src, dst) in enumerate((
        (scalar_hbm, scalar), (rows_hbm, rows_m), (ex_hbm, ex_m), (xy_hbm, xy_m),
        (xz_hbm, xz_m), (ey_hbm, ey_m), (eyt_hbm, eyt_m),
    )):
        load = pltpu.make_async_copy(src, dst, local_sem.at[i])
        load.start()
        loads.append(load)

    def remote(src, dst, send, recv, p, g):
        return pltpu.make_async_remote_copy(
            src_ref=src, dst_ref=dst, send_sem=send, recv_sem=recv,
            device_id={"gz": p, "gy": g}, device_id_type=pl.DeviceIdType.MESH,
        )

    def ux_copies(step):
        p = lax.rem(h + step, gz)
        planes = vel.at[0, pl.ds(p * nz, nz)]
        first = (
            pltpu.make_async_copy(planes, own.at[h], own_r.at[h])
            if step == 0
            else remote(planes, own.at[h], own_s.at[step], own_r.at[h], p, s)
        )
        return first, remote(planes, nxt.at[h], nxt_s.at[step], nxt_r.at[h], p, behind)

    ux = [ux_copies(step) for step in range(gz)]
    for first, second in ux:
        second.start()
        first.start()

    lane = lax.broadcasted_iota(jnp.int32, (yc, LANES), 1)
    for p in range(gz):
        planes = [vel[1, p * nz + z] for z in range(nz)]
        for z in range(p * nz - 1, p * nz + nz + 1):
            planes.append(vel[2, z] if 0 <= z < total else None)
        for c in range(per):
            tile = jnp.zeros((yc, LANES), jnp.float32)
            for i, plane in enumerate(planes):
                if plane is not None:
                    tile = jnp.where(
                        (lane >= i * bc) & (lane < (i + 1) * bc), roll(plane, (i - c) * bc, 1), tile
                    )
            vsend[p, c] = tile

    def v_copies(which, n, act, own_too):
        dst_buf, send, recv, back = ((v0, v0_s, v0_r, 0), (v1, v1_s, v1_r, 1))[which]
        p = n // per
        c = n % per
        g = lax.rem(h * per + c + gy - back, gy)
        mine = (p == h) & (g == s)

        @pl.when(jnp.logical_not(mine))
        def _():
            act(remote(vsend.at[p, c], dst_buf.at[s], send.at[n], recv.at[s], p, g))

        if own_too:
            @pl.when(mine)
            def _():
                act(pltpu.make_async_copy(vsend.at[p, c], dst_buf.at[s], recv.at[s]))

    for n in range(gz * per):
        for which in range(2):
            v_copies(which, n, lambda copy: copy.start(), True)

    loads[0].wait()
    loads[1].wait()
    loads[2].wait()
    count = nz * yc
    speed = None
    for i in range(gz):
        pltpu.make_async_copy(own.at[i], own.at[i], own_r.at[i]).wait()
        pltpu.make_async_copy(nxt.at[i], nxt.at[i], nxt_r.at[i]).wait()
        coarse = jnp.concatenate(
            [own[i].reshape(count, LANES), nxt[i].reshape(count, LANES)], axis=0
        )
        part = dot(dot(rows_m[...], coarse), ex_m[i])
        speed = part if speed is None else speed + part
    nx = scalar.shape[2]
    field = scalar[...].reshape(nz * rf, nx)
    field = sweep_periodic(field, speed, 1)

    wide = lax.broadcasted_iota(jnp.int32, (rf, LANES), 1)
    for g in range(gy):
        low = g * bf
        first, last = low // LANES, (low + bf - 1) // LANES
        tile = jnp.zeros((rf, LANES), jnp.float32)
        for z in range(nz):
            for t in range(first, last + 1):
                piece = field[z * rf : (z + 1) * rf, t * LANES : (t + 1) * LANES]
                begin = z * bf + max(0, t * LANES - low)
                end = z * bf + min(bf, (t + 1) * LANES - low)
                tile = jnp.where(
                    (wide >= begin) & (wide < end), roll(piece, z * bf - low, 1), tile
                )
        blocks[g] = tile

    def block_copy(step):
        g = lax.rem(s + step, gy)
        if step == 0:
            return pltpu.make_async_copy(blocks.at[g], pencil.at[s], blk_r.at[s])
        return remote(blocks.at[g], pencil.at[s], blk_s.at[step], blk_r.at[s], h, g)

    sends = [block_copy(step) for step in range(gy)]
    for copy in sends[1:] + sends[:1]:
        copy.start()

    for load in loads[3:]:
        load.wait()
    for i in range(gy):
        pltpu.make_async_copy(v0.at[i], v0.at[i], v0_r.at[i]).wait()
        pltpu.make_async_copy(v1.at[i], v1.at[i], v1_r.at[i]).wait()
    nyc = gy * yc
    coarse = jnp.concatenate(
        [v0[...].reshape(nyc, LANES), v1[...].reshape(nyc, LANES)], axis=1
    )
    speed_y = dot(eyt_m[...], dot(coarse, xy_m[...]))
    speed_z = dot(dot(xz_m[...], coarse, ((1,), (1,))), ey_m[...])

    for i in range(gy):
        pltpu.make_async_copy(pencil.at[i], pencil.at[i], blk_r.at[i]).wait()
    field = pencil[...].reshape(gy * rf, LANES)
    field = sweep_periodic(field, speed_y, 0)

    field = jnp.transpose(field)[: nz * bf]
    moved = displacement(
        speed_z[bf : (nz + 1) * bf], speed_z[: nz * bf], speed_z[2 * bf : (nz + 2) * bf]
    )
    w = weights(moved)

    def landing(target):
        result = None
        for m in range(-3, 4):
            z = target - m
            if 0 <= z < nz:
                at = slice(z * bf, (z + 1) * bf)
                term = field[at] * w[m][at]
                result = term if result is None else result + term
        return result

    for i in range(3):
        up_out[i] = landing(nz + i)
        down_out[i] = landing(i - 3)

    up = remote(up_out, up_in, z_s.at[0], z_r.at[0], lax.rem(h + 1, gz), s)
    down = remote(down_out, down_in, z_s.at[1], z_r.at[1], lax.rem(h + gz - 1, gz), s)

    @pl.when(h < gz - 1)
    def _():
        up.start()

    @pl.when(h > 0)
    def _():
        down.start()

    for i in range(nz):
        out[i] = landing(i)

    @pl.when(h > 0)
    def _():
        up.wait_recv()
        for i in range(3):
            out[i] = out[i] + up_in[i]
        down.wait_send()

    @pl.when(h < gz - 1)
    def _():
        down.wait_recv()
        for i in range(3):
            out[nz - 3 + i] = out[nz - 3 + i] + down_in[i]
        up.wait_send()

    for step, (first, second) in enumerate(ux):
        if step:
            first.wait_send()
        second.wait_send()
    for copy in sends[1:]:
        copy.wait_send()
    for n in range(gz * per):
        for which in range(2):
            v_copies(which, n, lambda copy: copy.wait_send(), False)


def local(scalar, velocity):
    gz, gy = lax.axis_size("gz"), lax.axis_size("gy")
    nz, rf, nx = scalar.shape
    yc, xc = velocity.shape[2:]
    bc = gz * xc // gy
    bf = 3 * bc
    ny = gy * rf
    vel = jnp.pad(velocity, ((0, 0), (0, 0), (0, 0), (0, LANES - xc)))
    mats = constants(nz, gz, gy, yc, xc)
    per = gy // gz
    f32 = jnp.float32
    dma = pltpu.SemaphoreType.DMA
    anywhere = pl.BlockSpec(memory_space=pl.ANY)
    vmem = pl.BlockSpec(memory_space=pltpu.VMEM)
    scratch = [pltpu.VMEM(scalar.shape, f32)]
    scratch += [pltpu.VMEM(m.shape, f32) for m in mats]
    scratch += [
        pltpu.VMEM((gz, nz, yc, LANES), f32),
        pltpu.VMEM((gz, nz, yc, LANES), f32),
        pltpu.VMEM((gz, per, yc, LANES), f32),
        pltpu.VMEM((gy, yc, LANES), f32),
        pltpu.VMEM((gy, yc, LANES), f32),
        pltpu.VMEM((gy, rf, LANES), f32),
        pltpu.VMEM((gy, rf, LANES), f32),
    ]
    scratch += [pltpu.VMEM((3, bf, ny), f32)] * 4
    scratch += [dma((n,)) for n in (
        1 + len(mats), gz, gz, gz, gz, gz * per, gy, gz * per, gy, gy, gy, 2, 2
    )]
    return pl.pallas_call(
        functools.partial(kernel, gz, gy, nz, yc, xc),
        out_shape=jax.ShapeDtypeStruct((nz, bf, ny), f32),
        in_specs=[anywhere, vmem] + [anywhere] * len(mats),
        out_specs=vmem,
        scratch_shapes=scratch,
        compiler_params=pltpu.CompilerParams(has_side_effects=True),
    )(scalar, vel, *[jnp.asarray(m) for m in mats])


def solution(mesh):
    in_specs = (P("gz", "gy", None), P(None, None, "gy", "gz"))
    out_specs = P("gz", "gy", None)
    return jax.shard_map(local, mesh=mesh, in_specs=in_specs, out_specs=out_specs, check_vma=False)
```

```python
import functools

import jax
import jax.numpy as jnp
import numpy as np
from jax import lax
from jax.experimental import pallas as pl
from jax.experimental.pallas import tpu as pltpu
from jax.sharding import PartitionSpec as P

LANES = 128
INNER = [1.0, 0.0, -5.0 / 4.0, -35.0 / 12.0, 21.0 / 4.0, -25.0 / 12.0]
MIDDLE = [-4.0, 75.0 / 4.0, -245.0 / 8.0, 545.0 / 24.0, -63.0 / 8.0, 25.0 / 24.0]
OUTER = [18.0, -153.0 / 4.0, 255.0 / 8.0, -313.0 / 24.0, 21.0 / 8.0, -5.0 / 24.0]


def shifted(factors, base, slope):
    total = np.polynomial.Polynomial([0.0])
    for factor in reversed(factors):
        total = total * np.polynomial.Polynomial([base, slope]) + factor
    coefs = np.zeros(6)
    coefs[: len(total.coef)] = total.coef
    return [0.0 if abs(c) < 1e-10 else float(c) for c in coefs]


AHEAD = {1: shifted(INNER, 1.0, -1.0), 2: shifted(MIDDLE, 2.0, -1.0), 3: shifted(OUTER, 3.0, -1.0)}
BEHIND = {1: shifted(MIDDLE, 1.0, 1.0), 2: shifted(OUTER, 2.0, 1.0)}


def horner(factors, value):
    lowest = 0
    while factors[lowest] == 0.0:
        lowest += 1
    result = jnp.full_like(value, factors[-1])
    for factor in reversed(factors[lowest:-1]):
        result = result * value
        if factor != 0.0:
            result = result + factor
    for _ in range(lowest):
        result = result * value
    return result


def weights(moved):
    size = jnp.abs(moved)
    positive = moved >= 0.0
    result = {0: horner(INNER, size)}
    for m in (1, 2, 3):
        near = horner(AHEAD[m], size)
        far = horner(BEHIND[m], size) if m in BEHIND else jnp.zeros_like(size)
        result[m] = jnp.where(positive, near, far)
        result[-m] = jnp.where(positive, far, near)
    return result


def displacement(speed, before, after):
    return speed + 0.5 * speed * jnp.where(speed >= 0.0, after - speed, speed - before)


def roll(value, shift, axis):
    return pltpu.roll(value, shift % value.shape[axis], axis)


def sweep_periodic(field, speed, axis):
    moved = displacement(speed, roll(speed, 1, axis), roll(speed, -1, axis))
    w = weights(moved)
    result = field * w[0]
    for m in (-3, -2, -1, 1, 2, 3):
        result = result + roll(field * w[m], m, axis)
    return result


def dot(a, b, dims=((1,), (0,))):
    return lax.dot_general(
        a, b, (dims, ((), ())), precision=lax.Precision.HIGHEST, preferred_element_type=jnp.float32
    )


def refine(coarse):
    out = np.zeros((coarse, 3 * coarse), np.float32)
    for c in range(coarse):
        for k in range(3):
            out[c, 3 * c + k] += 1.0 - k / 3.0
            out[(c + 1) % coarse, 3 * c + k] += k / 3.0
    return out


def refine_block(count):
    out = np.zeros((2 * count, 3 * count), np.float32)
    for c in range(count):
        for k in range(3):
            out[c, 3 * c + k] += 1.0 - k / 3.0
            out[c + 1, 3 * c + k] += k / 3.0
    return out


def constants(nz, gz, gy, yc, xc):
    bc = gz * xc // gy
    full = refine(gz * xc)
    ex = full.reshape(gz, xc, -1)
    block = refine_block(yc)
    rows = np.zeros((nz * 3 * yc, 2 * nz * yc), np.float32)
    for z in range(nz):
        for part in range(2):
            at = part * nz * yc + z * yc
            rows[z * 3 * yc : (z + 1) * 3 * yc, at : at + yc] = block[part * yc : (part + 1) * yc].T
    block = refine_block(bc)
    planes = 2 * nz + 2
    xy = np.zeros((2 * LANES, LANES), np.float32)
    xz = np.zeros(((nz + 2) * 3 * bc, 2 * LANES), np.float32)
    for plane in range(planes):
        for part in range(2):
            at = part * LANES + plane * bc
            piece = block[part * bc : (part + 1) * bc]
            if plane < nz:
                xy[at : at + bc, plane * 3 * bc : (plane + 1) * 3 * bc] = piece
            else:
                z = plane - nz
                xz[z * 3 * bc : (z + 1) * 3 * bc, at : at + bc] = piece.T
    ey = refine(gy * yc)
    return rows, ex, xy, xz, ey, np.ascontiguousarray(ey.T)


def kernel(gz, gy, nz, yc, xc, *refs):
    (scalar_hbm, vel_hbm, rows_hbm, ex_hbm, xy_hbm, xz_hbm, ey_hbm, eyt_hbm, out,
     scalar, vel, rows_m, ex_m, xy_m, xz_m, ey_m, eyt_m,
     own, nxt, vsend, v0, v1, blocks, pencil, up_out, down_out, up_in, down_in,
     local_sem, own_s, own_r, nxt_s, nxt_r, v0_s, v0_r, v1_s, v1_r, blk_s, blk_r, z_s, z_r) = refs
    h = lax.axis_index("gz")
    s = lax.axis_index("gy")
    rf = 3 * yc
    bc = gz * xc // gy
    bf = 3 * bc
    per = gy // gz
    ahead = lax.rem(s + 1, gy)
    behind = lax.rem(s + gy - 1, gy)
    total = gz * nz

    loads = []
    for i, (src, dst) in enumerate((
        (vel_hbm, vel), (scalar_hbm, scalar), (rows_hbm, rows_m), (ex_hbm, ex_m), (xy_hbm, xy_m),
        (xz_hbm, xz_m), (ey_hbm, ey_m), (eyt_hbm, eyt_m),
    )):
        load = pltpu.make_async_copy(src, dst, local_sem.at[i])
        load.start()
        loads.append(load)

    barrier = pltpu.get_barrier_semaphore()
    everyone = gz * gy

    def greet(i, _):
        other = lax.rem(h * gy + s + i, everyone)
        pl.semaphore_signal(
            barrier, inc=1, device_id={"gz": other // gy, "gy": lax.rem(other, gy)},
            device_id_type=pl.DeviceIdType.MESH,
        )
        return 0

    lax.fori_loop(1, everyone, greet, 0)

    def remote(src, dst, send, recv, p, g):
        return pltpu.make_async_remote_copy(
            src_ref=src, dst_ref=dst, send_sem=send, recv_sem=recv,
            device_id={"gz": p, "gy": g}, device_id_type=pl.DeviceIdType.MESH,
        )

    def ux_copies(step):
        p = lax.rem(h + step, gz)
        planes = vel.at[0, pl.ds(p * nz, nz)]
        first = (
            pltpu.make_async_copy(planes, own.at[h], own_r.at[h])
            if step == 0
            else remote(planes, own.at[h], own_s.at[step], own_r.at[h], p, s)
        )
        return first, remote(planes, nxt.at[h], nxt_s.at[step], nxt_r.at[h], p, behind)

    loads[0].wait()
    lane = lax.broadcasted_iota(jnp.int32, (yc, LANES), 1)
    fill = jnp.zeros((yc, LANES - xc), jnp.float32)
    def wide_plane(value):
        return jnp.concatenate([value, fill], axis=1)

    for p in range(gz):
        planes = [wide_plane(vel[1, p * nz + z]) for z in range(nz)]
        for z in range(p * nz - 1, p * nz + nz + 1):
            planes.append(wide_plane(vel[2, z]) if 0 <= z < total else None)
        for c in range(per):
            tile = jnp.zeros((yc, LANES), jnp.float32)
            for i, plane in enumerate(planes):
                if plane is not None:
                    tile = jnp.where(
                        (lane >= i * bc) & (lane < (i + 1) * bc), roll(plane, (i - c) * bc, 1), tile
                    )
            vsend[p, c] = tile

    pl.semaphore_wait(barrier, everyone - 1)
    ux = [ux_copies(step) for step in range(gz)]
    for first, second in ux:
        second.start()
        first.start()

    def v_copies(which, n, act, own_too):
        dst_buf, send, recv, back = ((v0, v0_s, v0_r, 0), (v1, v1_s, v1_r, 1))[which]
        p = n // per
        c = n % per
        g = lax.rem(h * per + c + gy - back, gy)
        mine = (p == h) & (g == s)

        @pl.when(jnp.logical_not(mine))
        def _():
            act(remote(vsend.at[p, c], dst_buf.at[s], send.at[n], recv.at[s], p, g))

        if own_too:
            @pl.when(mine)
            def _():
                act(pltpu.make_async_copy(vsend.at[p, c], dst_buf.at[s], recv.at[s]))

    for n in range(gz * per):
        for which in range(2):
            v_copies(which, n, lambda copy: copy.start(), True)

    for load in loads[1:4]:
        load.wait()
    count = nz * yc
    speed = None
    for i in range(gz):
        pltpu.make_async_copy(own.at[i], own.at[i], own_r.at[i]).wait()
        pltpu.make_async_copy(nxt.at[i], nxt.at[i], nxt_r.at[i]).wait()
        coarse = jnp.concatenate(
            [own[i].reshape(count, xc), nxt[i].reshape(count, xc)], axis=0
        )
        part = dot(dot(rows_m[...], coarse), ex_m[i])
        speed = part if speed is None else speed + part
    nx = scalar.shape[2]
    field = scalar[...].reshape(nz * rf, nx)
    field = sweep_periodic(field, speed, 1)

    wide = lax.broadcasted_iota(jnp.int32, (rf, LANES), 1)
    for g in range(gy):
        low = g * bf
        first, last = low // LANES, (low + bf - 1) // LANES
        tile = jnp.zeros((rf, LANES), jnp.float32)
        for z in range(nz):
            for t in range(first, last + 1):
                piece = field[z * rf : (z + 1) * rf, t * LANES : (t + 1) * LANES]
                begin = z * bf + max(0, t * LANES - low)
                end = z * bf + min(bf, (t + 1) * LANES - low)
                tile = jnp.where(
                    (wide >= begin) & (wide < end), roll(piece, z * bf - low, 1), tile
                )
        blocks[g] = tile

    def block_copy(step):
        g = lax.rem(s + step, gy)
        if step == 0:
            return pltpu.make_async_copy(blocks.at[g], pencil.at[s], blk_r.at[s])
        return remote(blocks.at[g], pencil.at[s], blk_s.at[step], blk_r.at[s], h, g)

    sends = [block_copy(step) for step in range(gy)]
    for copy in sends[1:] + sends[:1]:
        copy.start()

    for load in loads[4:]:
        load.wait()
    for i in range(gy):
        pltpu.make_async_copy(v0.at[i], v0.at[i], v0_r.at[i]).wait()
        pltpu.make_async_copy(v1.at[i], v1.at[i], v1_r.at[i]).wait()
    nyc = gy * yc
    coarse = jnp.concatenate(
        [v0[...].reshape(nyc, LANES), v1[...].reshape(nyc, LANES)], axis=1
    )
    speed_y = dot(eyt_m[...], dot(coarse, xy_m[...]))
    speed_z = dot(dot(xz_m[...], coarse, ((1,), (1,))), ey_m[...])

    for i in range(gy):
        pltpu.make_async_copy(pencil.at[i], pencil.at[i], blk_r.at[i]).wait()
    field = pencil[...].reshape(gy * rf, LANES)
    field = sweep_periodic(field, speed_y, 0)

    field = jnp.transpose(field)[: nz * bf]
    moved = displacement(
        speed_z[bf : (nz + 1) * bf], speed_z[: nz * bf], speed_z[2 * bf : (nz + 2) * bf]
    )
    w = weights(moved)

    def landing(target):
        result = None
        for m in range(-3, 4):
            z = target - m
            if 0 <= z < nz:
                at = slice(z * bf, (z + 1) * bf)
                term = field[at] * w[m][at]
                result = term if result is None else result + term
        return result

    for i in range(3):
        up_out[i] = landing(nz + i)
        down_out[i] = landing(i - 3)

    up = remote(up_out, up_in, z_s.at[0], z_r.at[0], lax.rem(h + 1, gz), s)
    down = remote(down_out, down_in, z_s.at[1], z_r.at[1], lax.rem(h + gz - 1, gz), s)

    @pl.when(h < gz - 1)
    def _():
        up.start()

    @pl.when(h > 0)
    def _():
        down.start()

    for i in range(nz):
        out[i] = landing(i)

    @pl.when(h > 0)
    def _():
        up.wait_recv()
        for i in range(3):
            out[i] = out[i] + up_in[i]
        down.wait_send()

    @pl.when(h < gz - 1)
    def _():
        down.wait_recv()
        for i in range(3):
            out[nz - 3 + i] = out[nz - 3 + i] + down_in[i]
        up.wait_send()

    for step, (first, second) in enumerate(ux):
        if step:
            first.wait_send()
        second.wait_send()
    for copy in sends[1:]:
        copy.wait_send()
    for n in range(gz * per):
        for which in range(2):
            v_copies(which, n, lambda copy: copy.wait_send(), False)


def local(scalar, velocity):
    gz, gy = lax.axis_size("gz"), lax.axis_size("gy")
    nz, rf, nx = scalar.shape
    yc, xc = velocity.shape[2:]
    bc = gz * xc // gy
    bf = 3 * bc
    ny = gy * rf
    mats = constants(nz, gz, gy, yc, xc)
    per = gy // gz
    f32 = jnp.float32
    dma = pltpu.SemaphoreType.DMA
    anywhere = pl.BlockSpec(memory_space=pl.ANY)
    vmem = pl.BlockSpec(memory_space=pltpu.VMEM)
    scratch = [pltpu.VMEM(scalar.shape, f32), pltpu.VMEM(velocity.shape, f32)]
    scratch += [pltpu.VMEM(m.shape, f32) for m in mats]
    scratch += [
        pltpu.VMEM((gz, nz, yc, xc), f32),
        pltpu.VMEM((gz, nz, yc, xc), f32),
        pltpu.VMEM((gz, per, yc, LANES), f32),
        pltpu.VMEM((gy, yc, LANES), f32),
        pltpu.VMEM((gy, yc, LANES), f32),
        pltpu.VMEM((gy, rf, LANES), f32),
        pltpu.VMEM((gy, rf, LANES), f32),
    ]
    scratch += [pltpu.VMEM((3, bf, ny), f32)] * 4
    scratch += [dma((n,)) for n in (
        2 + len(mats), gz, gz, gz, gz, gz * per, gy, gz * per, gy, gy, gy, 2, 2
    )]
    return pl.pallas_call(
        functools.partial(kernel, gz, gy, nz, yc, xc),
        out_shape=pltpu.VMEM((nz, bf, ny), f32),
        in_specs=[anywhere] * (2 + len(mats)),
        out_specs=vmem,
        scratch_shapes=scratch,
        compiler_params=pltpu.CompilerParams(has_side_effects=True, collective_id=0),
    )(scalar, velocity, *[jnp.asarray(m) for m in mats])


def solution(mesh):
    in_specs = (P("gz", "gy", None), P(None, None, "gy", "gz"))
    out_specs = P("gz", "gy", None)
    return jax.shard_map(local, mesh=mesh, in_specs=in_specs, out_specs=out_specs, check_vma=False)
```

```python
import functools

import jax
import jax.numpy as jnp
import numpy as np
from jax import lax
from jax.experimental import pallas as pl
from jax.experimental.pallas import tpu as pltpu
from jax.sharding import PartitionSpec as P

LANES = 128
INNER = [1.0, 0.0, -5.0 / 4.0, -35.0 / 12.0, 21.0 / 4.0, -25.0 / 12.0]
MIDDLE = [-4.0, 75.0 / 4.0, -245.0 / 8.0, 545.0 / 24.0, -63.0 / 8.0, 25.0 / 24.0]
OUTER = [18.0, -153.0 / 4.0, 255.0 / 8.0, -313.0 / 24.0, 21.0 / 8.0, -5.0 / 24.0]


def shifted(factors, base, slope):
    total = np.polynomial.Polynomial([0.0])
    for factor in reversed(factors):
        total = total * np.polynomial.Polynomial([base, slope]) + factor
    coefs = np.zeros(6)
    coefs[: len(total.coef)] = total.coef
    return [0.0 if abs(c) < 1e-10 else float(c) for c in coefs]


AHEAD = {1: shifted(INNER, 1.0, -1.0), 2: shifted(MIDDLE, 2.0, -1.0), 3: shifted(OUTER, 3.0, -1.0)}
BEHIND = {1: shifted(MIDDLE, 1.0, 1.0), 2: shifted(OUTER, 2.0, 1.0)}


def horner(factors, value):
    lowest = 0
    while factors[lowest] == 0.0:
        lowest += 1
    result = jnp.full_like(value, factors[-1])
    for factor in reversed(factors[lowest:-1]):
        result = result * value
        if factor != 0.0:
            result = result + factor
    for _ in range(lowest):
        result = result * value
    return result


def weights(moved):
    size = jnp.abs(moved)
    positive = moved >= 0.0
    result = {0: horner(INNER, size)}
    for m in (1, 2, 3):
        near = horner(AHEAD[m], size)
        far = horner(BEHIND[m], size) if m in BEHIND else jnp.zeros_like(size)
        result[m] = jnp.where(positive, near, far)
        result[-m] = jnp.where(positive, far, near)
    return result


def displacement(speed, before, after):
    return speed + 0.5 * speed * jnp.where(speed >= 0.0, after - speed, speed - before)


def roll(value, shift, axis):
    return pltpu.roll(value, shift % value.shape[axis], axis)


def sweep_periodic(field, speed, axis):
    moved = displacement(speed, roll(speed, 1, axis), roll(speed, -1, axis))
    w = weights(moved)
    result = field * w[0]
    for m in (-3, -2, -1, 1, 2, 3):
        result = result + roll(field * w[m], m, axis)
    return result


def dot(a, b, dims=((1,), (0,))):
    return lax.dot_general(
        a, b, (dims, ((), ())), precision=lax.Precision.HIGHEST, preferred_element_type=jnp.float32
    )


def refine(coarse):
    out = np.zeros((coarse, 3 * coarse), np.float32)
    for c in range(coarse):
        for k in range(3):
            out[c, 3 * c + k] += 1.0 - k / 3.0
            out[(c + 1) % coarse, 3 * c + k] += k / 3.0
    return out


def refine_block(count):
    out = np.zeros((2 * count, 3 * count), np.float32)
    for c in range(count):
        for k in range(3):
            out[c, 3 * c + k] += 1.0 - k / 3.0
            out[c + 1, 3 * c + k] += k / 3.0
    return out


def constants(nz, gz, gy, yc, xc):
    bc = gz * xc // gy
    full = refine(gz * xc)
    ex = full.reshape(gz, xc, -1)
    block = refine_block(yc)
    rows = np.zeros((nz * 3 * yc, 2 * nz * yc), np.float32)
    for z in range(nz):
        for part in range(2):
            at = part * nz * yc + z * yc
            rows[z * 3 * yc : (z + 1) * 3 * yc, at : at + yc] = block[part * yc : (part + 1) * yc].T
    block = refine_block(bc)
    planes = 2 * nz + 2
    xy = np.zeros((2 * LANES, LANES), np.float32)
    xz = np.zeros(((nz + 2) * 3 * bc, 2 * LANES), np.float32)
    for plane in range(planes):
        for part in range(2):
            at = part * LANES + plane * (bc + 1)
            piece = block[bc : bc + 1] if part else block[: bc + 1]
            end = at + len(piece)
            if plane < nz:
                xy[at:end, plane * 3 * bc : (plane + 1) * 3 * bc] = piece
            else:
                z = plane - nz
                xz[z * 3 * bc : (z + 1) * 3 * bc, at:end] = piece.T
    ey = refine(gy * yc)
    return rows, ex, xy, xz, ey, np.ascontiguousarray(ey.T)


def wrapped(index, size):
    return jnp.where(index >= size, index - size, index)


def kernel(gz, gy, nz, yc, xc, *refs):
    (scalar_hbm, vel_hbm, rows_hbm, ex_hbm, xy_hbm, xz_hbm, ey_hbm, eyt_hbm, out,
     scalar, vel, rows_m, ex_m, xy_m, xz_m, ey_m, eyt_m,
     own, nxt, vsend, v0, v1, blocks, pencil, up_out, down_out, up_in, down_in,
     local_sem, own_s, own_r, nxt_s, nxt_r, v0_s, v0_r, v1_s, v1_r, blk_s, blk_r, z_s, z_r) = refs
    h = lax.axis_index("gz")
    s = lax.axis_index("gy")
    rf = 3 * yc
    bc = gz * xc // gy
    bf = 3 * bc
    per = gy // gz
    behind = wrapped(s + gy - 1, gy)
    at_end = lax.rem(s, per) == per - 1
    total = gz * nz

    loads = []
    for i, (src, dst) in enumerate((
        (vel_hbm, vel), (scalar_hbm, scalar), (rows_hbm, rows_m), (ex_hbm, ex_m), (xy_hbm, xy_m),
        (xz_hbm, xz_m), (ey_hbm, ey_m), (eyt_hbm, eyt_m),
    )):
        load = pltpu.make_async_copy(src, dst, local_sem.at[i])
        load.start()
        loads.append(load)

    barrier = pltpu.get_barrier_semaphore()
    everyone = gz * gy

    def greet(step, p):
        pl.semaphore_signal(
            barrier, inc=1, device_id={"gz": p, "gy": wrapped(s + step, gy)},
            device_id_type=pl.DeviceIdType.MESH,
        )

    def greet_all(step, _):
        for i in range(gz):
            greet(step, wrapped(h + i, gz))
        return 0

    for i in range(1, gz):
        greet(0, wrapped(h + i, gz))
    lax.fori_loop(1, gy, greet_all, 0, unroll=gz * gy <= 64)

    def remote(src, dst, send, recv, p, g):
        return pltpu.make_async_remote_copy(
            src_ref=src, dst_ref=dst, send_sem=send, recv_sem=recv,
            device_id={"gz": p, "gy": g}, device_id_type=pl.DeviceIdType.MESH,
        )

    def ux_copies(step):
        p = wrapped(h + step, gz)
        planes = vel.at[0, pl.ds(p * nz, nz)]
        first = (
            pltpu.make_async_copy(planes, own.at[h], own_r.at[h])
            if step == 0
            else remote(planes, own.at[h], own_s.at[step], own_r.at[h], p, s)
        )
        return first, remote(planes, nxt.at[h], nxt_s.at[step], nxt_r.at[h], p, behind)

    loads[0].wait()
    lane = lax.broadcasted_iota(jnp.int32, (yc, LANES), 1)
    fill = jnp.zeros((yc, LANES - xc), jnp.float32)
    def wide_plane(value):
        return jnp.concatenate([value, fill], axis=1)

    for p in range(gz):
        planes = [wide_plane(vel[1, p * nz + z]) for z in range(nz)]
        for z in range(p * nz - 1, p * nz + nz + 1):
            planes.append(wide_plane(vel[2, z]) if 0 <= z < total else None)
        for c in range(per):
            tile = jnp.zeros((yc, LANES), jnp.float32)
            for i, plane in enumerate(planes):
                if plane is not None:
                    tile = jnp.where(
                        (lane >= i * (bc + 1)) & (lane < i * (bc + 1) + min(bc + 1, xc - c * bc)),
                        roll(plane, i * (bc + 1) - c * bc, 1),
                        tile,
                    )
            vsend[p, c] = tile


    @pl.when(jnp.logical_not(at_end))
    def _():
        v1[...] = jnp.zeros(v1.shape, jnp.float32)

    pl.semaphore_wait(barrier, everyone - 1)
    ux = [ux_copies(step) for step in range(gz)]
    for first, second in ux:
        second.start()
        first.start()

    def v_copies(p, c, first, act, own_too):
        if first:
            dst_buf, send, recv, g = v0, v0_s.at[p * per + c], v0_r, h * per + c
        else:
            dst_buf, send, recv, g = v1, v1_s.at[p], v1_r, wrapped(h * per + c + gy - 1, gy)
        mine = (p == h) & (g == s)

        @pl.when(jnp.logical_not(mine))
        def _():
            act(remote(vsend.at[p, c], dst_buf.at[s], send, recv.at[s], p, g))

        if own_too:
            @pl.when(mine)
            def _():
                act(pltpu.make_async_copy(vsend.at[p, c], dst_buf.at[s], recv.at[s]))

    v_tiles = [(p, c, first) for p in range(gz) for first in (True, False)
               for c in (range(per) if first else range(1))]
    for p, c, first in v_tiles:
        v_copies(p, c, first, lambda copy: copy.start(), True)

    for load in loads[1:4]:
        load.wait()
    count = nz * yc
    speed = None
    for i in range(gz):
        pltpu.make_async_copy(own.at[i], own.at[i], own_r.at[i]).wait()
        pltpu.make_async_copy(nxt.at[i], nxt.at[i], nxt_r.at[i]).wait()
        coarse = jnp.concatenate(
            [own[i].reshape(count, xc), nxt[i].reshape(count, xc)], axis=0
        )
        part = dot(dot(rows_m[...], coarse), ex_m[i])
        speed = part if speed is None else speed + part
    nx = scalar.shape[2]
    field = scalar[...].reshape(nz * rf, nx)
    field = sweep_periodic(field, speed, 1)

    wide = lax.broadcasted_iota(jnp.int32, (rf, LANES), 1)
    for g in range(gy):
        low = g * bf
        first, last = low // LANES, (low + bf - 1) // LANES
        tile = jnp.zeros((rf, LANES), jnp.float32)
        for z in range(nz):
            for t in range(first, last + 1):
                piece = field[z * rf : (z + 1) * rf, t * LANES : (t + 1) * LANES]
                begin = z * bf + max(0, t * LANES - low)
                end = z * bf + min(bf, (t + 1) * LANES - low)
                tile = jnp.where(
                    (wide >= begin) & (wide < end), roll(piece, z * bf - low, 1), tile
                )
        blocks[g] = tile

    def block_copy(step):
        g = wrapped(s + step, gy)
        if step == 0:
            return pltpu.make_async_copy(blocks.at[g], pencil.at[s], blk_r.at[s])
        return remote(blocks.at[g], pencil.at[s], blk_s.at[step], blk_r.at[s], h, g)

    sends = [block_copy(step) for step in range(gy)]
    for copy in sends[1:] + sends[:1]:
        copy.start()

    for load in loads[4:]:
        load.wait()
    for i in range(gy):
        pltpu.make_async_copy(v0.at[i], v0.at[i], v0_r.at[i]).wait()

    @pl.when(at_end)
    def _():
        for i in range(gy):
            pltpu.make_async_copy(v1.at[i], v1.at[i], v1_r.at[i]).wait()

    nyc = gy * yc
    coarse = jnp.concatenate(
        [v0[...].reshape(nyc, LANES), v1[...].reshape(nyc, LANES)], axis=1
    )
    speed_y = dot(eyt_m[...], dot(coarse, xy_m[...]))
    speed_z = dot(dot(xz_m[...], coarse, ((1,), (1,))), ey_m[...])

    for i in range(gy):
        pltpu.make_async_copy(pencil.at[i], pencil.at[i], blk_r.at[i]).wait()
    field = pencil[...].reshape(gy * rf, LANES)
    field = sweep_periodic(field, speed_y, 0)

    ny = gy * rf
    chunks = ny // LANES
    below, above = wrapped(h + gz - 1, gz), wrapped(h + 1, gz)
    ups, downs = [], []
    for k in range(chunks):
        cols = slice(k * LANES, (k + 1) * LANES)
        part = jnp.transpose(field[cols])[: nz * bf]
        moved = displacement(
            speed_z[bf : (nz + 1) * bf, cols], speed_z[: nz * bf, cols], speed_z[2 * bf :, cols]
        )
        w = weights(moved)

        def landing(target):
            result = None
            for m in range(-3, 4):
                z = target - m
                if 0 <= z < nz:
                    at = slice(z * bf, (z + 1) * bf)
                    term = part[at] * w[m][at]
                    result = term if result is None else result + term
            return result

        for i in range(3):
            up_out[k, i] = landing(nz + i)
            down_out[k, i] = landing(i - 3)
        up = remote(up_out.at[k], up_in.at[k], z_s.at[0, k], z_r.at[0, k], above, s)
        down = remote(down_out.at[k], down_in.at[k], z_s.at[1, k], z_r.at[1, k], below, s)
        ups.append(up)
        downs.append(down)

        @pl.when(h < gz - 1)
        def _():
            up.start()

        @pl.when(h > 0)
        def _():
            down.start()

        for i in range(nz):
            out[i, :, cols] = landing(i)

    @pl.when(h > 0)
    def _():
        for k in range(chunks):
            cols = slice(k * LANES, (k + 1) * LANES)
            ups[k].wait_recv()
            for i in range(3):
                out[i, :, cols] = out[i, :, cols] + up_in[k, i]
        for copy in downs:
            copy.wait_send()

    @pl.when(h < gz - 1)
    def _():
        for k in range(chunks):
            cols = slice(k * LANES, (k + 1) * LANES)
            downs[k].wait_recv()
            for i in range(nz - 3, nz):
                out[i, :, cols] = out[i, :, cols] + down_in[k, i - nz + 3]
        for copy in ups:
            copy.wait_send()

    for step, (first, second) in enumerate(ux):
        if step:
            first.wait_send()
        second.wait_send()
    for copy in sends[1:]:
        copy.wait_send()
    for p, c, first in v_tiles:
        v_copies(p, c, first, lambda copy: copy.wait_send(), False)


def local(scalar, velocity):
    gz, gy = lax.axis_size("gz"), lax.axis_size("gy")
    nz, rf, nx = scalar.shape
    yc, xc = velocity.shape[2:]
    bc = gz * xc // gy
    bf = 3 * bc
    ny = gy * rf
    mats = constants(nz, gz, gy, yc, xc)
    per = gy // gz
    f32 = jnp.float32
    dma = pltpu.SemaphoreType.DMA
    anywhere = pl.BlockSpec(memory_space=pl.ANY)
    vmem = pl.BlockSpec(memory_space=pltpu.VMEM)
    scratch = [pltpu.VMEM(scalar.shape, f32), pltpu.VMEM(velocity.shape, f32)]
    scratch += [pltpu.VMEM(m.shape, f32) for m in mats]
    scratch += [
        pltpu.VMEM((gz, nz, yc, xc), f32),
        pltpu.VMEM((gz, nz, yc, xc), f32),
        pltpu.VMEM((gz, per, yc, LANES), f32),
        pltpu.VMEM((gy, yc, LANES), f32),
        pltpu.VMEM((gy, yc, LANES), f32),
        pltpu.VMEM((gy, rf, LANES), f32),
        pltpu.VMEM((gy, rf, LANES), f32),
    ]
    scratch += [pltpu.VMEM((ny // LANES, 3, bf, LANES), f32)] * 4
    scratch += [dma((n,)) for n in (
        2 + len(mats), gz, gz, gz, gz, gz * per, gy, gz, gy, gy, gy
    )]
    scratch += [dma((2, ny // LANES))] * 2
    return pl.pallas_call(
        functools.partial(kernel, gz, gy, nz, yc, xc),
        out_shape=pltpu.VMEM((nz, bf, ny), f32),
        in_specs=[anywhere] * (2 + len(mats)),
        out_specs=vmem,
        scratch_shapes=scratch,
        compiler_params=pltpu.CompilerParams(has_side_effects=True, collective_id=0),
    )(scalar, velocity, *[jnp.asarray(m) for m in mats])


def solution(mesh):
    in_specs = (P("gz", "gy", None), P(None, None, "gy", "gz"))
    out_specs = P("gz", "gy", None)
    return jax.shard_map(local, mesh=mesh, in_specs=in_specs, out_specs=out_specs, check_vma=False)
```
